32 devices in a mesh: dp: 4 (over y, x), mp: 8 (over z, core).
Axes of the slice: x: 2, y: 2, z: 4, core: 2. Of those that a mesh axis runs over, the one named last changes fastest.
Arguments:
- query_grads: bfloat16 [4, 1, 3584, 4096], P('dp', None, None, 'mp'), may hold values from -102 to 102
- merge_grads: bfloat16 [4, 1, 4096, 3584], P('dp', None, 'mp'), may hold values from -102 to 102
- query_accum: float32 [1, 3584, 4096], P(None, 'dp', 'mp'), may hold values from -406 to 406
- merge_accum: float32 [1, 4096, 3584], P(None, 'mp', 'dp'), may hold values from -406 to 406
- query_master: float32 [1, 3584, 4096], P(None, 'dp', 'mp'), may hold values from -0.75 to 0.75
- merge_master: float32 [1, 4096, 3584], P(None, 'mp', 'dp'), may hold values from -0.75 to 0.75
- query_moment: float32 [1, 3584, 4096], P(None, 'dp', 'mp'), may hold values from -6 to 6
- merge_moment: float32 [1, 4096, 3584], P(None, 'mp', 'dp'), may hold values from -6 to 6
- query_second: float32 [1, 3584, 4096], P(None, 'dp', 'mp'), may hold values from 0.3 to 3
- merge_second: float32 [1, 4096, 3584], P(None, 'mp', 'dp'), may hold values from 0.3 to 3
Outputs:
- query_weight: bfloat16 [1, 3584, 4096], P(None, None, 'mp')
- merge_weight: bfloat16 [1, 4096, 3584], P(None, 'mp')
- query_shard: float32 [1, 3584, 4096], P(None, 'dp', 'mp')
- merge_shard: float32 [1, 4096, 3584], P(None, 'mp', 'dp')
- query_first: float32 [1, 3584, 4096], P(None, 'dp', 'mp')
- merge_first: float32 [1, 4096, 3584], P(None, 'mp', 'dp')
- query_variance: float32 [1, 3584, 4096], P(None, 'dp', 'mp')
- merge_variance: float32 [1, 4096, 3584], P(None, 'mp', 'dp')
The draws below stay inside these ranges and needn't reach their ends.
All inputs are finite; a program needn't handle non-finite values.
Results may differ from the reference program's by a relative error of at most 0.0015.
Values may be sent and summed in bfloat16 or wider, within the bound.
No kernel may reach another device: no remote copies, remote signals or barrier semaphores. Data moves between devices by JAX's collectives and lax.ppermute only.
A program may use at most 128 MiB of HBM per device.

```python
import math
import jax
import jax.numpy as jnp
from jax import lax

D = 3584
HEADS = 16
HEAD_DIM = 256
LAYERS = 1
STEP = 10
QW = 4096
ENTRIES = 29360128
N_DP = 4


def scaled_field(key, tag, noise_tag, shape, base):
    rows = shape[-2]
    cols = shape[-1]
    scale_key = jax.random.fold_in(key, tag)
    row_rise = 1.0 + 0.75 * jnp.arange(rows, dtype=jnp.float32)[:, None] / rows
    col_rise = 1.0 + 0.75 * jnp.arange(cols, dtype=jnp.float32)[None, :] / cols
    row_shape = tuple(shape[:-1]) + (1,)
    col_shape = tuple(shape[:-2]) + (1, cols)
    row_scale = jnp.exp(jax.random.uniform(jax.random.fold_in(scale_key, 1), row_shape, jnp.float32) * math.log(10.0)) * row_rise
    col_scale = jnp.exp(jax.random.uniform(jax.random.fold_in(scale_key, 2), col_shape, jnp.float32) * math.log(10.0)) * col_rise
    noise_key = jax.random.fold_in(key, noise_tag)
    value = jax.random.truncated_normal(noise_key, -4.0, 4.0, shape, jnp.float32)
    return base * value * row_scale * col_scale


def draw_query_grads(key, part):
    return scaled_field(key, 1, 5, (N_DP, LAYERS, D, HEADS * HEAD_DIM), 0.05).astype(jnp.bfloat16)


def draw_merge_grads(key, part):
    return scaled_field(key, 2, 6, (N_DP, LAYERS, HEADS * HEAD_DIM, D), 0.05).astype(jnp.bfloat16)


def draw_query_accum(key, part):
    return scaled_field(key, 3, 7, (LAYERS, D, HEADS * HEAD_DIM), 0.2)


def draw_merge_accum(key, part):
    return scaled_field(key, 4, 8, (LAYERS, HEADS * HEAD_DIM, D), 0.2)


def block_scale(key, extent, split, smallest, largest):
    level, own = 1.0, jax.random.fold_in(key, 6)
    for position, parts in split:
        draws = jnp.exp(jax.random.uniform(jax.random.fold_in(own, position), (parts,), jnp.float32, smallest / len(split), largest / len(split)))
        level = level * jnp.repeat(draws, extent[position] // parts).reshape([-1 if axis == position else 1 for axis in range(len(extent))])
    return level


def bell_draw(rng, shape, scale, most, pieces=(), kind=jnp.bfloat16):
    drawn = jax.random.normal(rng, shape, jnp.float32) * scale
    if len(pieces) > 0:
        drawn = block_scale(rng, shape, pieces, -0.22, 0.18) * drawn
    return jnp.clip(drawn, min=-most, max=most).astype(kind)


def setup_inputs(seed: int = 0) -> dict:
    key_of = jax.random.split(jax.random.key(seed), 11)
    return {
        "query_grads": draw_query_grads(jax.random.fold_in(key_of[10], 71), 0),
        "merge_grads": draw_merge_grads(jax.random.fold_in(key_of[10], 71), 0),
        "query_accum": draw_query_accum(jax.random.fold_in(key_of[10], 71), 0),
        "merge_accum": draw_merge_accum(jax.random.fold_in(key_of[10], 71), 0),
        "query_master": bell_draw(key_of[4], (LAYERS, D, QW), 0.05, 0.75, ((1, 4), (2, 8)), jnp.float32),
        "merge_master": bell_draw(key_of[5], (LAYERS, QW, D), 0.05, 0.75, ((1, 8), (2, 4)), jnp.float32),
        "query_moment": bell_draw(key_of[6], (LAYERS, D, QW), 1.0, 6.0, ((1, 4), (2, 8)), jnp.float32),
        "merge_moment": bell_draw(key_of[7], (LAYERS, QW, D), 1.0, 6.0, ((1, 8), (2, 4)), jnp.float32),
        "query_second": jnp.clip(jnp.exp(math.log(3.0) - 2.3025851 * jax.random.uniform(key_of[8], (LAYERS, D, QW), jnp.float32) ** block_scale(key_of[8], (LAYERS, D, QW), ((1, 4), (2, 8)), -0.2, 0.2)), 0.3, 3.0),
        "merge_second": jnp.clip(jnp.exp(math.log(3.0) - 2.3025851 * jax.random.uniform(key_of[9], (LAYERS, QW, D), jnp.float32) ** block_scale(key_of[9], (LAYERS, QW, D), ((1, 8), (2, 4)), -0.2, 0.2)), 0.3, 3.0),
    }


beta_one = 0.9
beta_two = 0.95
learn_rate = 0.002
weight_decay = 0.1
adam_eps = 1e-08

def adamw(total, clip, master, moment, second):
    scaled = clip * total
    first = beta_one * moment + (1.0 - beta_one) * scaled
    variance = beta_two * second + (1.0 - beta_two) * scaled * scaled
    corr_one = 1.0 - beta_one ** STEP
    corr_two = 1.0 - beta_two ** STEP
    update = first / corr_one / (jnp.sqrt(variance / corr_two) + adam_eps) + weight_decay * master
    return (master - learn_rate * update, first, variance)

def reference(query_grads, merge_grads, query_accum, merge_accum, query_master, merge_master, query_moment, merge_moment, query_second, merge_second):
    query_total = query_accum + lax.optimization_barrier(jnp.sum(query_grads.astype(jnp.float32), axis=0))
    merge_total = merge_accum + lax.optimization_barrier(jnp.sum(merge_grads.astype(jnp.float32), axis=0))
    sumsq = jnp.sum(query_total * query_total) + jnp.sum(merge_total * merge_total)
    clip = jnp.minimum(1.0, lax.rsqrt(sumsq / float(ENTRIES) + 1e-06))
    query_shard, query_first, query_variance = adamw(query_total, clip, query_master, query_moment, query_second)
    merge_shard, merge_first, merge_variance = adamw(merge_total, clip, merge_master, merge_moment, merge_second)
    return (query_shard.astype(jnp.bfloat16), merge_shard.astype(jnp.bfloat16), query_shard, merge_shard, query_first, merge_first, query_variance, merge_variance)
```

```python
import functools

import jax
import jax.numpy as jnp
from jax import lax
from jax.experimental import pallas as pl
from jax.experimental.pallas import tpu as pltpu
from jax.sharding import PartitionSpec as P

STEP = 10

beta_one = 0.9
beta_two = 0.95
learn_rate = 0.002
weight_decay = 0.1
adam_eps = 1e-08

BLOCKS = 4
HEAD = 1


def adamw(total, clip, master, moment, second):
    scaled = clip * total
    first = beta_one * moment + (1.0 - beta_one) * scaled
    variance = beta_two * second + (1.0 - beta_two) * scaled * scaled
    corr_one = 1.0 - beta_one**STEP
    corr_two = 1.0 - beta_two**STEP
    update = first * (1.0 / corr_one) / (jnp.sqrt(variance * (1.0 / corr_two)) + adam_eps)
    return (master - learn_rate * (update + weight_decay * master), first, variance)


class Layout:
    def __init__(self, rows, cols, axis, parts):
        self.rows, self.cols, self.axis, self.parts = rows, cols, axis, parts
        self.step = rows // BLOCKS
        self.block = (self.step, cols)
        self.whole = (rows * parts, cols) if axis == 0 else (rows, cols * parts)

    def piece(self, partner, start=0):
        def index(i):
            owner = lax.axis_index("dp") ^ partner
            return (owner * BLOCKS + start + i, 0) if self.axis == 0 else (start + i, owner)

        return pl.BlockSpec(self.block, index)

    def shard(self, start=0):
        return pl.BlockSpec(self.block, lambda i: (start + i, 0))

    def short(self):
        return pl.BlockSpec(self.block, lambda i: (jnp.minimum(i, HEAD - 1), 0))

    def long(self):
        return pl.BlockSpec(self.block, lambda i: (jnp.maximum(i - HEAD, 0), 0))

    def array(self, blocks, dtype):
        return jax.ShapeDtypeStruct((blocks * self.step, self.cols), dtype)

    def bytes(self, blocks, width):
        return blocks * self.step * self.cols * width


def call(body, grid, in_specs, out_specs, out_shape, cost, aliases=None, name=None):
    return pl.pallas_call(
        body,
        grid=(grid,),
        in_specs=in_specs,
        out_specs=out_specs,
        out_shape=out_shape,
        input_output_aliases=aliases or {},
        compiler_params=pltpu.CompilerParams(
            dimension_semantics=("arbitrary",), vmem_limit_bytes=24 * 2**20
        ),
        cost_estimate=pl.CostEstimate(flops=cost * 2, bytes_accessed=cost, transcendentals=0),
        name=name,
    )


def copy_body(source, target):
    target[...] = source[...]


def extract(lay, grads, partner):
    return call(
        copy_body,
        BLOCKS,
        [lay.piece(partner)],
        lay.shard(),
        lay.array(BLOCKS, jnp.bfloat16),
        lay.bytes(BLOCKS, 4),
        name="extract",
    )(grads)


def add_body(grads, arrived, short, long):
    value = (grads[...].astype(jnp.float32) + arrived[...].astype(jnp.float32)).astype(jnp.bfloat16)
    i = pl.program_id(0)

    @pl.when(i < HEAD)
    def _():
        short[...] = value

    @pl.when(i >= HEAD)
    def _():
        long[...] = value


def add_forward(lay, grads, arrived, partner):
    return call(
        add_body,
        BLOCKS,
        [lay.piece(partner), lay.shard()],
        [lay.short(), lay.long()],
        [lay.array(HEAD, jnp.bfloat16), lay.array(BLOCKS - HEAD, jnp.bfloat16)],
        lay.bytes(BLOCKS, 6),
        name="add_forward",
    )(grads, arrived)


def partial_body(grads, arrived, accum, out):
    out[...] = accum[...] + (grads[...].astype(jnp.float32) + arrived[...].astype(jnp.float32))


def partial_sum(lay, grads, arrived, accum):
    return call(
        partial_body,
        BLOCKS,
        [lay.piece(0), lay.shard(), lay.shard()],
        lay.shard(),
        lay.array(BLOCKS, jnp.float32),
        lay.bytes(BLOCKS, 12),
        name="partial_sum",
    )(grads, arrived, accum)


def squares(held, arrived):
    total = held[...] + arrived[...].astype(jnp.float32)
    rows, cols = total.shape
    tile = jnp.sum((total * total).reshape(rows // 8, 8, cols), axis=0)
    return sum(tile[:, k : k + 128] for k in range(0, cols, 128))


def long_body(held, arrived, out):
    @pl.when(pl.program_id(0) == 0)
    def _():
        out[...] = jnp.zeros_like(out)

    out[...] += squares(held, arrived)


def long_squares(lay, held, arrived):
    n = BLOCKS - HEAD
    return call(
        long_body,
        n,
        [lay.shard(HEAD), lay.shard()],
        pl.BlockSpec((8, 128), lambda i: (0, 0)),
        jax.ShapeDtypeStruct((8, 128), jnp.float32),
        lay.bytes(n, 6),
        name="long_squares",
    )(held, arrived)


def short_body(held_one, arrived_one, held_two, arrived_two, sum_one, sum_two, out):
    value = squares(held_one, arrived_one) + squares(held_two, arrived_two)

    @pl.when(pl.program_id(0) == 0)
    def _():
        out[...] = jnp.broadcast_to(jnp.sum(sum_one[...] + sum_two[...], axis=0, keepdims=True), out.shape)

    out[...] += jnp.broadcast_to(jnp.sum(value, axis=0, keepdims=True), out.shape)


def short_squares(lays, helds, arriveds, sums, devices):
    tile = pl.BlockSpec((8, 128), lambda i: (0, 0))
    one, two = lays
    return call(
        short_body,
        HEAD,
        [one.shard(), one.shard(), two.shard(), two.shard(), tile, tile],
        pl.BlockSpec((devices, 128), lambda i: (0, 0)),
        jax.ShapeDtypeStruct((devices, 128), jnp.float32),
        one.bytes(HEAD, 12),
        name="short_squares",
    )(helds[0], arriveds[0], helds[1], arriveds[1], *sums)


def clip_of(entries, sums):
    sumsq = jnp.sum(jnp.sum(sums[...], axis=0, keepdims=True), axis=1, keepdims=True)
    return jnp.minimum(1.0, lax.rsqrt(sumsq / entries + 1e-06))


def weight_body(entries, sums, held, arrived, master, moment, second, out):
    total = held[...] + arrived[...].astype(jnp.float32)
    shard, _, _ = adamw(total, clip_of(entries, sums), master[...], moment[...], second[...])
    out[...] = shard.astype(jnp.bfloat16)


def weight_piece(lay, start, blocks, entries, sums, held, arrived, state):
    return call(
        functools.partial(weight_body, entries),
        blocks,
        [pl.BlockSpec(sums.shape, lambda i: (0, 0)), lay.shard(start), lay.shard()] + [lay.shard(start)] * 3,
        lay.shard(),
        lay.array(blocks, jnp.bfloat16),
        lay.bytes(blocks, 20),
        name="weight_piece",
    )(sums, held, arrived, *state)


def update_body(entries, sums, held, short, long, master, moment, second, shard_out, first_out, variance_out):
    arrived = jnp.where(
        pl.program_id(0) < HEAD, short[...].astype(jnp.float32), long[...].astype(jnp.float32)
    )
    shard, first, variance = adamw(
        held[...] + arrived, clip_of(entries, sums), master[...], moment[...], second[...]
    )
    shard_out[...] = shard
    first_out[...] = first
    variance_out[...] = variance


def update(lay, entries, sums, held, short, long, state):
    return call(
        functools.partial(update_body, entries),
        BLOCKS,
        [pl.BlockSpec(sums.shape, lambda i: (0, 0)), lay.shard(), lay.short(), lay.long()] + [lay.shard()] * 3,
        [lay.shard()] * 3,
        [lay.array(BLOCKS, jnp.float32)] * 3,
        lay.bytes(BLOCKS, 30),
        name="update",
    )(sums, held, short, long, *state)


def place_body(*refs):
    short, long, out = refs[-3:]
    out[...] = jnp.where(pl.program_id(0) < HEAD, short[...], long[...])


def place(lay, whole, short, long, partner):
    first = whole is None
    return call(
        place_body,
        BLOCKS,
        ([] if first else [pl.BlockSpec(memory_space=pl.ANY)]) + [lay.short(), lay.long()],
        lay.piece(partner),
        jax.ShapeDtypeStruct(lay.whole, jnp.bfloat16),
        lay.bytes(BLOCKS, 4),
        aliases=None if first else {0: 0},
        name="place",
    )(*([] if first else [whole]), short, long)


def place_long_body(_, long, out):
    out[...] = long[...]


def place_long(lay, whole, long, partner):
    return call(
        place_long_body,
        BLOCKS - HEAD,
        [pl.BlockSpec(memory_space=pl.ANY), lay.shard()],
        lay.piece(partner, HEAD),
        jax.ShapeDtypeStruct(lay.whole, jnp.bfloat16),
        lay.bytes(BLOCKS - HEAD, 4),
        aliases={0: 0},
        name="place_long",
    )(whole, long)


def place_short_body(_, __, one, two, out_one, out_two):
    out_one[...] = one[...]
    out_two[...] = two[...]


def place_short(lays, wholes, shorts, partner):
    one, two = lays
    hbm = pl.BlockSpec(memory_space=pl.ANY)
    return call(
        place_short_body,
        HEAD,
        [hbm, hbm, one.shard(), two.shard()],
        [one.piece(partner), two.piece(partner)],
        [jax.ShapeDtypeStruct(lay.whole, jnp.bfloat16) for lay in lays],
        one.bytes(HEAD, 8),
        aliases={0: 0, 1: 1},
        name="place_short",
    )(*wholes, *shorts)


def exchange(value, partner, parts):
    return lax.ppermute(value, "dp", [(i, i ^ partner) for i in range(parts)])


def on_square(parts, devices, entries, *args):
    grads = [a.reshape(a.shape[-2:]) for a in args[:2]]
    accums = [a.reshape(a.shape[-2:]) for a in args[2:4]]
    states = [[a.reshape(a.shape[-2:]) for a in args[4 + k :: 2]] for k in range(2)]
    lays = [Layout(*accums[k].shape, k, parts) for k in range(2)]
    near, far = (1, 2), (2, 1)
    both = range(2)

    relayed = [exchange(extract(lays[k], grads[k], 3), near[k], parts) for k in both]
    direct = [exchange(extract(lays[k], grads[k], near[k]), near[k], parts) for k in both]
    sent = [add_forward(lays[k], grads[k], relayed[k], far[k]) for k in both]
    long = [exchange(sent[k][1], far[k], parts) for k in both]
    short = [exchange(sent[k][0], far[k], parts) for k in both]
    held = [partial_sum(lays[k], grads[k], direct[k], accums[k]) for k in both]
    sums = [long_squares(lays[k], held[k], long[k]) for k in both]
    sums = short_squares(lays, held, short, sums, devices)
    sums = lax.all_to_all(sums, ("dp", "mp"), 0, 0, tiled=True)

    own_short = [weight_piece(lays[k], 0, HEAD, entries, sums, held[k], short[k], states[k]) for k in both]
    near_short = [exchange(own_short[k], near[k], parts) for k in both]
    own_long = [
        weight_piece(lays[k], HEAD, BLOCKS - HEAD, entries, sums, held[k], long[k], states[k]) for k in both
    ]
    near_long = [exchange(own_long[k], near[k], parts) for k in both]
    far_long = [exchange(own_long[k], far[k], parts) for k in both]
    far_short = [exchange(own_short[k], far[k], parts) for k in both]
    last_long = [exchange(near_long[k], far[k], parts) for k in both]
    last_short = [exchange(near_short[k], far[k], parts) for k in both]

    updated = [update(lays[k], entries, sums, held[k], short[k], long[k], states[k]) for k in both]
    wholes = [place(lays[k], None, own_short[k], own_long[k], 0) for k in both]
    wholes = [place(lays[k], wholes[k], near_short[k], near_long[k], near[k]) for k in both]
    wholes = [place(lays[k], wholes[k], far_short[k], far_long[k], far[k]) for k in both]
    wholes = [place_long(lays[k], wholes[k], last_long[k], 3) for k in both]
    wholes = place_short(lays, wholes, last_short, 3)
    return tuple(w[None] for w in wholes) + tuple(updated[k][j][None] for j in range(3) for k in both)


def on_any(entries, *args):
    grads, accums = args[:2], args[2:4]
    states = [args[4 + k :: 2] for k in range(2)]
    axes = (1, 2)
    totals = [
        accums[k]
        + lax.psum_scatter(grads[k][0], "dp", scatter_dimension=axes[k], tiled=True).astype(jnp.float32)
        for k in range(2)
    ]
    sumsq = lax.psum(sum(jnp.sum(t * t) for t in totals), ("dp", "mp"))
    clip = jnp.minimum(1.0, lax.rsqrt(sumsq / entries + 1e-06))
    updated = [adamw(totals[k], clip, *states[k]) for k in range(2)]
    weights = tuple(
        lax.all_gather(updated[k][0].astype(jnp.bfloat16), "dp", axis=axes[k], tiled=True) for k in range(2)
    )
    return weights + tuple(updated[k][j] for j in range(3) for k in range(2))


def solution(mesh):
    parts = mesh.shape["dp"]
    devices = mesh.size

    def on_device(*args):
        entries = float(devices * sum(a.size for a in args[2:4]))
        tiled = all(a.shape[-2] % (16 * BLOCKS) == 0 and a.shape[-1] % 128 == 0 for a in args[2:4])
        if parts == 4 and tiled:
            return on_square(parts, devices, entries, *args)
        return on_any(entries, *args)

    rows, cols = P(None, "dp", "mp"), P(None, "mp", "dp")
    return jax.shard_map(
        on_device,
        mesh=mesh,
        in_specs=(P("dp", None, None, "mp"), P("dp", None, "mp", None)) + (rows, cols) * 4,
        out_specs=(P(None, None, "mp"), P(None, "mp", None)) + (rows, cols) * 3,
        check_vma=False,
    )
```

```python
import functools

import jax
import jax.numpy as jnp
from jax import lax
from jax.experimental import pallas as pl
from jax.experimental.pallas import tpu as pltpu
from jax.sharding import PartitionSpec as P


STEP = 10

beta_one = 0.9
beta_two = 0.95
learn_rate = 0.002
weight_decay = 0.1
adam_eps = 1e-08

BLOCKS = 4
HEAD = 1


def adamw(total, clip, master, moment, second):
    scaled = clip * total
    first = beta_one * moment + (1.0 - beta_one) * scaled
    variance = beta_two * second + (1.0 - beta_two) * scaled * scaled
    corr_one = 1.0 - beta_one**STEP
    corr_two = 1.0 - beta_two**STEP
    update = first * (1.0 / corr_one) / (jnp.sqrt(variance * (1.0 / corr_two)) + adam_eps)
    return (master - learn_rate * (update + weight_decay * master), first, variance)


class Layout:
    def __init__(self, rows, cols, axis, parts):
        self.rows, self.cols, self.axis, self.parts = rows, cols, axis, parts
        self.step = rows // BLOCKS
        self.block = (self.step, cols)
        self.whole = (rows * parts, cols) if axis == 0 else (rows, cols * parts)

    def piece(self, partner, start=0):
        def index(i):
            owner = lax.axis_index("dp") ^ partner
            return (owner * BLOCKS + start + i, 0) if self.axis == 0 else (start + i, owner)

        return pl.BlockSpec(self.block, index)

    def shard(self, start=0):
        return pl.BlockSpec(self.block, lambda i: (start + i, 0))

    def short(self):
        return pl.BlockSpec(self.block, lambda i: (jnp.minimum(i, HEAD - 1), 0))

    def long(self):
        return pl.BlockSpec(self.block, lambda i: (jnp.maximum(i - HEAD, 0), 0))

    def array(self, blocks, dtype):
        return jax.ShapeDtypeStruct((blocks * self.step, self.cols), dtype)

    def bytes(self, blocks, width):
        return blocks * self.step * self.cols * width


def call(body, grid, in_specs, out_specs, out_shape, cost, aliases=None):
    return pl.pallas_call(
        body,
        grid=(grid,),
        in_specs=in_specs,
        out_specs=out_specs,
        out_shape=out_shape,
        input_output_aliases=aliases or {},
        compiler_params=pltpu.CompilerParams(
            dimension_semantics=("arbitrary",), vmem_limit_bytes=24 * 2**20
        ),
        cost_estimate=pl.CostEstimate(flops=cost * 2, bytes_accessed=cost, transcendentals=0),
    )


def copy_body(source, target):
    target[...] = source[...]


def extract(lay, grads, partner):
    return call(
        copy_body, BLOCKS, [lay.piece(partner)], lay.shard(), lay.array(BLOCKS, jnp.bfloat16), lay.bytes(BLOCKS, 4)
    )(grads)


def add_body(grads, arrived, short, long):
    value = (grads[...].astype(jnp.float32) + arrived[...].astype(jnp.float32)).astype(jnp.bfloat16)
    i = pl.program_id(0)

    @pl.when(i < HEAD)
    def _():
        short[...] = value

    @pl.when(i >= HEAD)
    def _():
        long[...] = value


def add_forward(lay, grads, arrived, partner):
    return call(
        add_body,
        BLOCKS,
        [lay.piece(partner), lay.shard()],
        [lay.short(), lay.long()],
        [lay.array(HEAD, jnp.bfloat16), lay.array(BLOCKS - HEAD, jnp.bfloat16)],
        lay.bytes(BLOCKS, 6),
    )(grads, arrived)


def partial_body(grads, arrived, accum, out):
    out[...] = accum[...] + (grads[...].astype(jnp.float32) + arrived[...].astype(jnp.float32))


def partial_sum(lay, grads, arrived, accum):
    return call(
        partial_body,
        BLOCKS,
        [lay.piece(0), lay.shard(), lay.shard()],
        lay.shard(),
        lay.array(BLOCKS, jnp.float32),
        lay.bytes(BLOCKS, 12),
    )(grads, arrived, accum)


def squares(held, arrived):
    total = held[...] + arrived[...].astype(jnp.float32)
    rows, cols = total.shape
    tile = jnp.sum((total * total).reshape(rows // 8, 8, cols), axis=0)
    return sum(tile[:, k : k + 128] for k in range(0, cols, 128))


def long_body(held, arrived, out):
    @pl.when(pl.program_id(0) == 0)
    def _():
        out[...] = jnp.zeros_like(out)

    out[...] += squares(held, arrived)


def long_squares(lay, held, arrived):
    n = BLOCKS - HEAD
    return call(
        long_body,
        n,
        [lay.shard(HEAD), lay.shard()],
        pl.BlockSpec((8, 128), lambda i: (0, 0)),
        jax.ShapeDtypeStruct((8, 128), jnp.float32),
        lay.bytes(n, 6),
    )(held, arrived)


def short_body(held_one, arrived_one, held_two, arrived_two, sum_one, sum_two, out):
    value = squares(held_one, arrived_one) + squares(held_two, arrived_two)

    @pl.when(pl.program_id(0) == 0)
    def _():
        out[...] = jnp.broadcast_to(jnp.sum(sum_one[...] + sum_two[...], axis=0, keepdims=True), out.shape)

    out[...] += jnp.broadcast_to(jnp.sum(value, axis=0, keepdims=True), out.shape)


def short_squares(lays, helds, arriveds, sums, devices):
    tile = pl.BlockSpec((8, 128), lambda i: (0, 0))
    one, two = lays
    return call(
        short_body,
        HEAD,
        [one.shard(), one.shard(), two.shard(), two.shard(), tile, tile],
        pl.BlockSpec((devices, 128), lambda i: (0, 0)),
        jax.ShapeDtypeStruct((devices, 128), jnp.float32),
        one.bytes(HEAD, 12),
    )(helds[0], arriveds[0], helds[1], arriveds[1], *sums)


def clip_of(entries, sums):
    sumsq = jnp.sum(jnp.sum(sums[...], axis=0, keepdims=True), axis=1, keepdims=True)
    return jnp.minimum(1.0, lax.rsqrt(sumsq / entries + 1e-06))


def weight_body(entries, sums, held, arrived, master, moment, second, out):
    total = held[...] + arrived[...].astype(jnp.float32)
    shard, _, _ = adamw(total, clip_of(entries, sums), master[...], moment[...], second[...])
    out[...] = shard.astype(jnp.bfloat16)


def weight_piece(lay, start, blocks, entries, sums, held, arrived, state):
    return call(
        functools.partial(weight_body, entries),
        blocks,
        [pl.BlockSpec(sums.shape, lambda i: (0, 0)), lay.shard(start), lay.shard()] + [lay.shard(start)] * 3,
        lay.shard(),
        lay.array(blocks, jnp.bfloat16),
        lay.bytes(blocks, 20),
    )(sums, held, arrived, *state)


def update_body(entries, sums, held, short, long, master, moment, second, shard_out, first_out, variance_out):
    arrived = jnp.where(
        pl.program_id(0) < HEAD, short[...].astype(jnp.float32), long[...].astype(jnp.float32)
    )
    shard, first, variance = adamw(
        held[...] + arrived, clip_of(entries, sums), master[...], moment[...], second[...]
    )
    shard_out[...] = shard
    first_out[...] = first
    variance_out[...] = variance


def update(lay, entries, sums, held, short, long, state):
    return call(
        functools.partial(update_body, entries),
        BLOCKS,
        [pl.BlockSpec(sums.shape, lambda i: (0, 0)), lay.shard(), lay.short(), lay.long()] + [lay.shard()] * 3,
        [lay.shard()] * 3,
        [lay.array(BLOCKS, jnp.float32)] * 3,
        lay.bytes(BLOCKS, 30),
    )(sums, held, short, long, *state)


def place_body(*refs):
    short, long, out = refs[-3:]
    out[...] = jnp.where(pl.program_id(0) < HEAD, short[...], long[...])


def place(lay, whole, short, long, partner):
    first = whole is None
    return call(
        place_body,
        BLOCKS,
        ([] if first else [pl.BlockSpec(memory_space=pl.ANY)]) + [lay.short(), lay.long()],
        lay.piece(partner),
        jax.ShapeDtypeStruct(lay.whole, jnp.bfloat16),
        lay.bytes(BLOCKS, 4),
        aliases=None if first else {0: 0},
    )(*([] if first else [whole]), short, long)


def place_long_body(_, long, out):
    out[...] = long[...]


def place_long(lay, whole, long, partner):
    return call(
        place_long_body,
        BLOCKS - HEAD,
        [pl.BlockSpec(memory_space=pl.ANY), lay.shard()],
        lay.piece(partner, HEAD),
        jax.ShapeDtypeStruct(lay.whole, jnp.bfloat16),
        lay.bytes(BLOCKS - HEAD, 4),
        aliases={0: 0},
    )(whole, long)


def place_short_body(_, __, one, two, out_one, out_two):
    out_one[...] = one[...]
    out_two[...] = two[...]


def place_short(lays, wholes, shorts, partner):
    one, two = lays
    hbm = pl.BlockSpec(memory_space=pl.ANY)
    return call(
        place_short_body,
        HEAD,
        [hbm, hbm, one.shard(), two.shard()],
        [one.piece(partner), two.piece(partner)],
        [jax.ShapeDtypeStruct(lay.whole, jnp.bfloat16) for lay in lays],
        one.bytes(HEAD, 8),
        aliases={0: 0, 1: 1},
    )(*wholes, *shorts)


def exchange(value, partner, parts):
    return lax.ppermute(value, "dp", [(i, i ^ partner) for i in range(parts)])


def on_square(parts, devices, entries, *args):
    grads = [a.reshape(a.shape[-2:]) for a in args[:2]]
    accums = [a.reshape(a.shape[-2:]) for a in args[2:4]]
    states = [[a.reshape(a.shape[-2:]) for a in args[4 + k :: 2]] for k in range(2)]
    lays = [Layout(*accums[k].shape, k, parts) for k in range(2)]
    near, far = (1, 2), (2, 1)
    both = range(2)

    def step(function, *lists):
        return [function(lays[k], *(x[k] for x in lists)) for k in both]

    def move(values, partners):
        return [exchange(values[k], partners[k], parts) for k in both]

    relayed = move(step(extract, grads, (3, 3)), near)
    direct = move(step(extract, grads, near), near)
    sent = step(add_forward, grads, relayed, far)
    tail = move([x[1] for x in sent], far)
    head = move([x[0] for x in sent], far)
    held = step(partial_sum, grads, direct, accums)
    sums = step(long_squares, held, tail)
    sums = short_squares(lays, held, head, sums, devices)
    sums = lax.all_to_all(sums, ("dp", "mp"), 0, 0, tiled=True)

    def weights(start, blocks):
        return lambda lay, held, arrived, state: weight_piece(lay, start, blocks, entries, sums, held, arrived, state)

    own_head = step(weights(0, HEAD), held, head, states)
    own_tail = step(weights(HEAD, BLOCKS - HEAD), held, tail, states)
    near_head, near_tail = move(own_head, near), move(own_tail, near)
    far_tail, far_head = move(own_tail, far), move(own_head, far)
    last_tail, last_head = move(near_tail, far), move(near_head, far)

    updated = step(lambda lay, *x: update(lay, entries, sums, *x), held, head, tail, states)
    wholes = step(place, (None, None), own_head, own_tail, (0, 0))
    wholes = step(place, wholes, near_head, near_tail, near)
    wholes = step(place, wholes, far_head, far_tail, far)
    wholes = step(place_long, wholes, last_tail, (3, 3))
    wholes = place_short(lays, wholes, last_head, 3)
    return tuple(w[None] for w in wholes) + tuple(updated[k][j][None] for j in range(3) for k in both)


def on_any(entries, *args):
    grads, accums = args[:2], args[2:4]
    states = [args[4 + k :: 2] for k in range(2)]
    axes = (1, 2)
    totals = [
        accums[k]
        + lax.psum_scatter(grads[k][0], "dp", scatter_dimension=axes[k], tiled=True).astype(jnp.float32)
        for k in range(2)
    ]
    sumsq = lax.psum(sum(jnp.sum(t * t) for t in totals), ("dp", "mp"))
    clip = jnp.minimum(1.0, lax.rsqrt(sumsq / entries + 1e-06))
    updated = [adamw(totals[k], clip, *states[k]) for k in range(2)]
    weights = tuple(
        lax.all_gather(updated[k][0].astype(jnp.bfloat16), "dp", axis=axes[k], tiled=True) for k in range(2)
    )
    return weights + tuple(updated[k][j] for j in range(3) for k in range(2))


def solution(mesh):
    parts = mesh.shape["dp"]
    devices = mesh.size

    def on_device(*args):
        entries = float(devices * sum(a.size for a in args[2:4]))
        tiled = all(a.shape[-2] % (16 * BLOCKS) == 0 and a.shape[-1] % 128 == 0 for a in args[2:4])
        if parts == 4 and tiled:
            return on_square(parts, devices, entries, *args)
        return on_any(entries, *args)

    rows, cols = P(None, "dp", "mp"), P(None, "mp", "dp")
    return jax.shard_map(
        on_device,
        mesh=mesh,
        in_specs=(P("dp", None, None, "mp"), P("dp", None, "mp", None)) + (rows, cols) * 4,
        out_specs=(P(None, None, "mp"), P(None, "mp", None)) + (rows, cols) * 3,
        check_vma=False,
    )
```

```python
import functools

import jax
import jax.numpy as jnp
from jax import lax
from jax.experimental import pallas as pl
from jax.experimental.pallas import tpu as pltpu
from jax.sharding import PartitionSpec as P


STEP = 10

beta_one = 0.9
beta_two = 0.95
learn_rate = 0.002
weight_decay = 0.1
adam_eps = 1e-08

BLOCKS = 4
HEAD = 1

CUT_GRANT = 8


def adamw(total, clip, master, moment, second):
    scaled = clip * total
    first = beta_one * moment + (1.0 - beta_one) * scaled
    variance = beta_two * second + (1.0 - beta_two) * scaled * scaled
    corr_one = 1.0 - beta_one**STEP
    corr_two = 1.0 - beta_two**STEP
    update = first * (1.0 / corr_one) / (jnp.sqrt(variance * (1.0 / corr_two)) + adam_eps)
    return (master - learn_rate * (update + weight_decay * master), first, variance)


KEEP = 1.0 - learn_rate * weight_decay
FIRST = learn_rate / (1.0 - beta_one**STEP)
SECOND = 1.0 / (1.0 - beta_two**STEP)


def shard_of(kept, pull, spread, scaled):
    step = pull + (FIRST * (1.0 - beta_one)) * scaled
    width = jnp.sqrt(spread + (SECOND * (1.0 - beta_two)) * (scaled * scaled)) + adam_eps
    return kept - step / width


class Layout:
    def __init__(self, rows, cols, axis, parts):
        self.rows, self.cols, self.axis, self.parts = rows, cols, axis, parts
        self.step = rows // BLOCKS
        self.block = (self.step, cols)
        self.whole = (rows * parts, cols) if axis == 0 else (rows, cols * parts)

    def piece(self, partner, start=0):
        def index(i):
            owner = lax.axis_index("dp") ^ partner
            return (owner * BLOCKS + start + i, 0) if self.axis == 0 else (start + i, owner)

        return pl.BlockSpec(self.block, index)

    def quarter(self, ref, owner):
        if self.axis == 0:
            return ref.at[pl.ds(pl.multiple_of(owner * self.rows, self.rows), self.rows), :]
        return ref.at[:, pl.ds(pl.multiple_of(owner * self.cols, self.cols), self.cols)]

    def shard(self, start=0):
        return pl.BlockSpec(self.block, lambda i: (start + i, 0))

    def short(self):
        return pl.BlockSpec(self.block, lambda i: (jnp.minimum(i, HEAD - 1), 0))

    def long(self):
        return pl.BlockSpec(self.block, lambda i: (jnp.maximum(i - HEAD, 0), 0))

    def array(self, blocks, dtype):
        return jax.ShapeDtypeStruct((blocks * self.step, self.cols), dtype)

    def bytes(self, blocks, width):
        return blocks * self.step * self.cols * width


def call(body, grid, in_specs, out_specs, out_shape, cost, aliases=None, grant=24):
    return pl.pallas_call(
        body,
        grid=(grid,),
        in_specs=in_specs,
        out_specs=out_specs,
        out_shape=out_shape,
        input_output_aliases=aliases or {},
        compiler_params=pltpu.CompilerParams(
            dimension_semantics=("arbitrary",), vmem_limit_bytes=grant * 2**20
        ),
        cost_estimate=pl.CostEstimate(flops=cost * 2, bytes_accessed=cost, transcendentals=0),
    )


def cut_body(lays, partners, grads_one, grads_two, out_one, out_two, sems):
    me = lax.axis_index("dp")
    copies = [
        pltpu.make_async_copy(lay.quarter(grads, me ^ partner), out, sems.at[k])
        for k, (lay, partner, grads, out) in enumerate(
            zip(lays, partners, (grads_one, grads_two), (out_one, out_two))
        )
    ]
    for copy in copies:
        copy.start()
    for copy in copies:
        copy.wait()


def cut(lays, grads, partners):
    size = sum(lay.bytes(BLOCKS, 2) for lay in lays)
    return pl.pallas_call(
        functools.partial(cut_body, lays, partners),
        in_specs=[pl.BlockSpec(memory_space=pltpu.HBM)] * 2,
        out_specs=[pl.BlockSpec(memory_space=pltpu.VMEM)] * 2,
        out_shape=[pltpu.VMEM((lay.rows, lay.cols), jnp.bfloat16) for lay in lays],
        scratch_shapes=[pltpu.SemaphoreType.DMA((2,))],
        compiler_params=pltpu.CompilerParams(vmem_limit_bytes=CUT_GRANT * 2**20),
        cost_estimate=pl.CostEstimate(flops=size, bytes_accessed=2 * size, transcendentals=0),
        name="cut",
    )(*(pltpu.with_memory_space_constraint(g, pltpu.HBM) for g in grads))


def add_body(grads, arrived, short, long):
    value = (grads[...].astype(jnp.float32) + arrived[...].astype(jnp.float32)).astype(jnp.bfloat16)
    i = pl.program_id(0)

    @pl.when(i < HEAD)
    def _():
        short[...] = value

    @pl.when(i >= HEAD)
    def _():
        long[...] = value


def add_forward(lay, grads, arrived, partner):
    return call(
        add_body,
        BLOCKS,
        [lay.piece(partner), lay.shard()],
        [lay.short(), lay.long()],
        [lay.array(HEAD, jnp.bfloat16), lay.array(BLOCKS - HEAD, jnp.bfloat16)],
        lay.bytes(BLOCKS, 6),
    )(grads, arrived)


def partial_body(grads, arrived, accum, out):
    out[...] = accum[...] + (grads[...].astype(jnp.float32) + arrived[...].astype(jnp.float32))


def partial_sum(lay, grads, arrived, accum):
    return call(
        partial_body,
        BLOCKS,
        [lay.piece(0), lay.shard(), lay.shard()],
        lay.shard(),
        lay.array(BLOCKS, jnp.float32),
        lay.bytes(BLOCKS, 12),
    )(grads, arrived, accum)


def ready_body(master, moment, second, kept, pull, spread):
    kept[...] = KEEP * master[...]
    pull[...] = (FIRST * beta_one) * moment[...]
    spread[...] = (SECOND * beta_two) * second[...]


def ready(lay, state):
    return call(
        ready_body,
        BLOCKS,
        [lay.shard()] * 3,
        [lay.shard()] * 3,
        [lay.array(BLOCKS, jnp.float32)] * 3,
        lay.bytes(BLOCKS, 24),
    )(*state)


def squares(held, arrived, out):
    total = held[...] + arrived[...].astype(jnp.float32)
    out[...] = total
    rows, cols = total.shape
    tile = jnp.sum((total * total).reshape(rows // 8, 8, cols), axis=0)
    return sum(tile[:, k : k + 128] for k in range(0, cols, 128))


def long_body(held, arrived, total, out):
    @pl.when(pl.program_id(0) == 0)
    def _():
        out[...] = jnp.zeros_like(out)

    out[...] += squares(held, arrived, total)


def long_squares(lay, held, arrived):
    n = BLOCKS - HEAD
    return call(
        long_body,
        n,
        [lay.shard(HEAD), lay.shard()],
        [lay.shard(), pl.BlockSpec((8, 128), lambda i: (0, 0))],
        [lay.array(n, jnp.float32), jax.ShapeDtypeStruct((8, 128), jnp.float32)],
        lay.bytes(n, 10),
    )(held, arrived)


def short_body(held_one, arrived_one, held_two, arrived_two, sum_one, sum_two, total_one, total_two, out):
    value = squares(held_one, arrived_one, total_one) + squares(held_two, arrived_two, total_two)

    @pl.when(pl.program_id(0) == 0)
    def _():
        out[...] = jnp.broadcast_to(jnp.sum(sum_one[...] + sum_two[...], axis=0, keepdims=True), out.shape)

    out[...] += jnp.broadcast_to(jnp.sum(value, axis=0, keepdims=True), out.shape)


def short_squares(lays, helds, arriveds, sums, devices):
    tile = pl.BlockSpec((8, 128), lambda i: (0, 0))
    one, two = lays
    *totals, sums = call(
        short_body,
        HEAD,
        [one.shard(), one.shard(), two.shard(), two.shard(), tile, tile],
        [one.shard(), two.shard(), pl.BlockSpec((devices, 128), lambda i: (0, 0))],
        [lay.array(HEAD, jnp.float32) for lay in lays] + [jax.ShapeDtypeStruct((devices, 128), jnp.float32)],
        one.bytes(HEAD, 20),
    )(helds[0], arriveds[0], helds[1], arriveds[1], *sums)
    return totals, sums


def clip_of(entries, sums):
    sumsq = jnp.sum(jnp.sum(sums[...], axis=0, keepdims=True), axis=1, keepdims=True)
    return jnp.minimum(1.0, lax.rsqrt(sumsq / entries + 1e-06))


def weight_body(entries, sums, total, kept, pull, spread, out):
    scaled = clip_of(entries, sums) * total[...]
    out[...] = shard_of(kept[...], pull[...], spread[...], scaled).astype(jnp.bfloat16)


def weight_piece(lay, start, blocks, entries, sums, total, terms):
    return call(
        functools.partial(weight_body, entries),
        blocks,
        [pl.BlockSpec(sums.shape, lambda i: (0, 0)), lay.shard()] + [lay.shard(start)] * 3,
        lay.shard(),
        lay.array(blocks, jnp.bfloat16),
        lay.bytes(blocks, 18),
    )(sums, total, *terms)


def update_body(entries, sums, short, long, master, moment, second, shard_out, first_out, variance_out):
    scaled = clip_of(entries, sums) * jnp.where(pl.program_id(0) < HEAD, short[...], long[...])
    shard_out[...] = shard_of(
        KEEP * master[...], (FIRST * beta_one) * moment[...], (SECOND * beta_two) * second[...], scaled
    )
    first_out[...] = beta_one * moment[...] + (1.0 - beta_one) * scaled
    variance_out[...] = beta_two * second[...] + (1.0 - beta_two) * (scaled * scaled)


def update(lay, entries, sums, short, long, state):
    return call(
        functools.partial(update_body, entries),
        BLOCKS,
        [pl.BlockSpec(sums.shape, lambda i: (0, 0)), lay.short(), lay.long()] + [lay.shard()] * 3,
        [lay.shard()] * 3,
        [lay.array(BLOCKS, jnp.float32)] * 3,
        lay.bytes(BLOCKS, 28),
    )(sums, short, long, *state)


def place_body(*refs):
    short, long, out = refs[-3:]
    out[...] = jnp.where(pl.program_id(0) < HEAD, short[...], long[...])


def place(lay, whole, short, long, partner):
    first = whole is None
    return call(
        place_body,
        BLOCKS,
        ([] if first else [pl.BlockSpec(memory_space=pl.ANY)]) + [lay.short(), lay.long()],
        lay.piece(partner),
        jax.ShapeDtypeStruct(lay.whole, jnp.bfloat16),
        lay.bytes(BLOCKS, 4),
        aliases=None if first else {0: 0},
    )(*([] if first else [whole]), short, long)


def place_long_body(_, long, out):
    out[...] = long[...]


def place_long(lay, whole, long, partner):
    return call(
        place_long_body,
        BLOCKS - HEAD,
        [pl.BlockSpec(memory_space=pl.ANY), lay.shard()],
        lay.piece(partner, HEAD),
        jax.ShapeDtypeStruct(lay.whole, jnp.bfloat16),
        lay.bytes(BLOCKS - HEAD, 4),
        aliases={0: 0},
    )(whole, long)


def place_short_body(_, __, one, two, out_one, out_two):
    out_one[...] = one[...]
    out_two[...] = two[...]


def place_short(lays, wholes, shorts, partner):
    one, two = lays
    hbm = pl.BlockSpec(memory_space=pl.ANY)
    return call(
        place_short_body,
        HEAD,
        [hbm, hbm, one.shard(), two.shard()],
        [one.piece(partner), two.piece(partner)],
        [jax.ShapeDtypeStruct(lay.whole, jnp.bfloat16) for lay in lays],
        one.bytes(HEAD, 8),
        aliases={0: 0, 1: 1},
    )(*wholes, *shorts)


def exchange(value, partner, parts):
    return lax.ppermute(value, "dp", [(i, i ^ partner) for i in range(parts)])


def on_square(parts, devices, entries, *args):
    grads = [a.reshape(a.shape[-2:]) for a in args[:2]]
    accums = [a.reshape(a.shape[-2:]) for a in args[2:4]]
    states = [[a.reshape(a.shape[-2:]) for a in args[4 + k :: 2]] for k in range(2)]
    lays = [Layout(*accums[k].shape, k, parts) for k in range(2)]
    near, far = (1, 2), (2, 1)
    both = range(2)

    def step(function, *lists):
        return [function(lays[k], *(x[k] for x in lists)) for k in both]

    def move(values, partners):
        return [exchange(values[k], partners[k], parts) for k in both]

    relayed = move(cut(lays, grads, (3, 3)), near)
    direct = move(cut(lays, grads, near), near)
    sent = step(add_forward, grads, relayed, far)
    tail = move([x[1] for x in sent], far)
    head = move([x[0] for x in sent], far)
    held = step(partial_sum, grads, direct, accums)
    terms = step(ready, states)
    tail_totals, sums = zip(*step(long_squares, held, tail))
    head_totals, sums = short_squares(lays, held, head, sums, devices)
    sums = lax.all_to_all(sums, ("dp", "mp"), 0, 0, tiled=True)

    def weights(start, blocks):
        return lambda lay, total, terms: weight_piece(lay, start, blocks, entries, sums, total, terms)

    own_head = step(weights(0, HEAD), head_totals, terms)
    own_tail = step(weights(HEAD, BLOCKS - HEAD), tail_totals, terms)
    near_head, near_tail = move(own_head, near), move(own_tail, near)
    far_tail, far_head = move(own_tail, far), move(own_head, far)
    last_tail, last_head = move(near_tail, far), move(near_head, far)

    updated = step(lambda lay, *x: update(lay, entries, sums, *x), head_totals, tail_totals, states)
    wholes = step(place, (None, None), own_head, own_tail, (0, 0))
    wholes = step(place, wholes, near_head, near_tail, near)
    wholes = step(place, wholes, far_head, far_tail, far)
    wholes = step(place_long, wholes, last_tail, (3, 3))
    wholes = place_short(lays, wholes, last_head, 3)
    return tuple(w[None] for w in wholes) + tuple(updated[k][j][None] for j in range(3) for k in both)


def on_any(entries, *args):
    grads, accums = args[:2], args[2:4]
    states = [args[4 + k :: 2] for k in range(2)]
    axes = (1, 2)
    totals = [
        accums[k]
        + lax.psum_scatter(grads[k][0], "dp", scatter_dimension=axes[k], tiled=True).astype(jnp.float32)
        for k in range(2)
    ]
    sumsq = lax.psum(sum(jnp.sum(t * t) for t in totals), ("dp", "mp"))
    clip = jnp.minimum(1.0, lax.rsqrt(sumsq / entries + 1e-06))
    updated = [adamw(totals[k], clip, *states[k]) for k in range(2)]
    weights = tuple(
        lax.all_gather(updated[k][0].astype(jnp.bfloat16), "dp", axis=axes[k], tiled=True) for k in range(2)
    )
    return weights + tuple(updated[k][j] for j in range(3) for k in range(2))


def solution(mesh):
    parts = mesh.shape["dp"]
    devices = mesh.size

    def on_device(*args):
        entries = float(devices * sum(a.size for a in args[2:4]))
        tiled = all(a.shape[-2] % (16 * BLOCKS) == 0 and a.shape[-1] % 128 == 0 for a in args[2:4])
        if parts == 4 and tiled:
            return on_square(parts, devices, entries, *args)
        return on_any(entries, *args)

    rows, cols = P(None, "dp", "mp"), P(None, "mp", "dp")
    return jax.shard_map(
        on_device,
        mesh=mesh,
        in_specs=(P("dp", None, None, "mp"), P("dp", None, "mp", None)) + (rows, cols) * 4,
        out_specs=(P(None, None, "mp"), P(None, "mp", None)) + (rows, cols) * 3,
        check_vma=False,
    )
```

```python
import functools

import jax
import jax.numpy as jnp
from jax import lax
from jax.experimental import pallas as pl
from jax.experimental.pallas import tpu as pltpu
from jax.sharding import PartitionSpec as P


STEP = 10

beta_one = 0.9
beta_two = 0.95
learn_rate = 0.002
weight_decay = 0.1
adam_eps = 1e-08

BLOCKS = 4
HEAD = 1

CUT_GRANT = 8


def adamw(total, clip, master, moment, second):
    scaled = clip * total
    first = beta_one * moment + (1.0 - beta_one) * scaled
    variance = beta_two * second + (1.0 - beta_two) * scaled * scaled
    corr_one = 1.0 - beta_one**STEP
    corr_two = 1.0 - beta_two**STEP
    update = first * (1.0 / corr_one) / (jnp.sqrt(variance * (1.0 / corr_two)) + adam_eps)
    return (master - learn_rate * (update + weight_decay * master), first, variance)


KEEP = 1.0 - learn_rate * weight_decay
FIRST = learn_rate / (1.0 - beta_one**STEP)
SECOND = 1.0 / (1.0 - beta_two**STEP)


def shard_of(kept, pull, spread, scaled):
    step = pull + (FIRST * (1.0 - beta_one)) * scaled
    width = jnp.sqrt(spread + (SECOND * (1.0 - beta_two)) * (scaled * scaled)) + adam_eps
    return kept - step / width


class Layout:
    def __init__(self, rows, cols, axis, parts):
        self.rows, self.cols, self.axis, self.parts = rows, cols, axis, parts
        self.step = rows // BLOCKS
        self.block = (self.step, cols)
        self.whole = (rows * parts, cols) if axis == 0 else (rows, cols * parts)

    def piece(self, partner, start=0):
        def index(i):
            owner = lax.axis_index("dp") ^ partner
            return (owner * BLOCKS + start + i, 0) if self.axis == 0 else (start + i, owner)

        return pl.BlockSpec(self.block, index)

    def quarter(self, ref, owner, start=0, blocks=BLOCKS):
        first, size = start * self.step, blocks * self.step
        if self.axis == 0:
            return ref.at[pl.ds(pl.multiple_of(owner * self.rows + first, self.step), size), :]
        return ref.at[pl.ds(first, size), pl.ds(pl.multiple_of(owner * self.cols, self.cols), self.cols)]

    def shard(self, start=0):
        return pl.BlockSpec(self.block, lambda i: (start + i, 0))

    def short(self):
        return pl.BlockSpec(self.block, lambda i: (jnp.minimum(i, HEAD - 1), 0))

    def long(self):
        return pl.BlockSpec(self.block, lambda i: (jnp.maximum(i - HEAD, 0), 0))

    def array(self, blocks, dtype):
        return jax.ShapeDtypeStruct((blocks * self.step, self.cols), dtype)

    def bytes(self, blocks, width):
        return blocks * self.step * self.cols * width


def call(body, grid, in_specs, out_specs, out_shape, cost, aliases=None, grant=24):
    return pl.pallas_call(
        body,
        grid=(grid,),
        in_specs=in_specs,
        out_specs=out_specs,
        out_shape=out_shape,
        input_output_aliases=aliases or {},
        compiler_params=pltpu.CompilerParams(
            dimension_semantics=("arbitrary",), vmem_limit_bytes=grant * 2**20
        ),
        cost_estimate=pl.CostEstimate(flops=cost * 2, bytes_accessed=cost, transcendentals=0),
    )


def cut_body(lays, partners, start, blocks, grads_one, grads_two, out_one, out_two, sems):
    me = lax.axis_index("dp")
    copies = [
        pltpu.make_async_copy(lay.quarter(grads, me ^ partner, start, blocks), out, sems.at[k])
        for k, (lay, partner, grads, out) in enumerate(
            zip(lays, partners, (grads_one, grads_two), (out_one, out_two))
        )
    ]
    for copy in copies:
        copy.start()
    for copy in copies:
        copy.wait()


def cut(lays, grads, partners, start=0, blocks=BLOCKS):
    size = sum(lay.bytes(blocks, 2) for lay in lays)
    return pl.pallas_call(
        functools.partial(cut_body, lays, partners, start, blocks),
        in_specs=[pl.BlockSpec(memory_space=pltpu.HBM)] * 2,
        out_specs=[pl.BlockSpec(memory_space=pl.ANY)] * 2,
        out_shape=[pltpu.VMEM((blocks * lay.step, lay.cols), jnp.bfloat16) for lay in lays],
        scratch_shapes=[pltpu.SemaphoreType.DMA((2,))],
        compiler_params=pltpu.CompilerParams(vmem_limit_bytes=CUT_GRANT * 2**20),
        cost_estimate=pl.CostEstimate(flops=size, bytes_accessed=2 * size, transcendentals=0),
        name="cut",
    )(*(pltpu.with_memory_space_constraint(g, pltpu.HBM) for g in grads))


def add_body(grads, arrived_short, arrived_long, short, long):
    i = pl.program_id(0)
    arrived = jnp.where(i < HEAD, arrived_short[...].astype(jnp.float32), arrived_long[...].astype(jnp.float32))
    value = (grads[...].astype(jnp.float32) + arrived).astype(jnp.bfloat16)

    @pl.when(i < HEAD)
    def _():
        short[...] = value

    @pl.when(i >= HEAD)
    def _():
        long[...] = value


def add_forward(lay, grads, short, long, partner):
    return call(
        add_body,
        BLOCKS,
        [lay.piece(partner), lay.short(), lay.long()],
        [lay.short(), lay.long()],
        [lay.array(HEAD, jnp.bfloat16), lay.array(BLOCKS - HEAD, jnp.bfloat16)],
        lay.bytes(BLOCKS, 6),
    )(grads, short, long)


def partial_body(grads, arrived, accum, out):
    out[...] = accum[...] + (grads[...].astype(jnp.float32) + arrived[...].astype(jnp.float32))


def partial_sum(lay, grads, arrived, accum):
    return call(
        partial_body,
        BLOCKS,
        [lay.piece(0), lay.shard(), lay.shard()],
        lay.shard(),
        lay.array(BLOCKS, jnp.float32),
        lay.bytes(BLOCKS, 12),
    )(grads, arrived, accum)


def ready_body(master, moment, second, kept, pull, spread):
    kept[...] = KEEP * master[...]
    pull[...] = (FIRST * beta_one) * moment[...]
    spread[...] = (SECOND * beta_two) * second[...]


def ready(lay, state):
    return call(
        ready_body,
        BLOCKS,
        [lay.shard()] * 3,
        [lay.shard()] * 3,
        [lay.array(BLOCKS, jnp.float32)] * 3,
        lay.bytes(BLOCKS, 24),
    )(*state)


def squares(held, arrived, out):
    total = held[...] + arrived[...].astype(jnp.float32)
    out[...] = total
    rows, cols = total.shape
    tile = jnp.sum((total * total).reshape(rows // 8, 8, cols), axis=0)
    return sum(tile[:, k : k + 128] for k in range(0, cols, 128))


def long_body(held, arrived, total, out):
    @pl.when(pl.program_id(0) == 0)
    def _():
        out[...] = jnp.zeros_like(out)

    out[...] += squares(held, arrived, total)


def long_squares(lay, held, arrived):
    n = BLOCKS - HEAD
    return call(
        long_body,
        n,
        [lay.shard(HEAD), lay.shard()],
        [lay.shard(), pl.BlockSpec((8, 128), lambda i: (0, 0))],
        [lay.array(n, jnp.float32), jax.ShapeDtypeStruct((8, 128), jnp.float32)],
        lay.bytes(n, 10),
    )(held, arrived)


def short_body(held_one, arrived_one, held_two, arrived_two, sum_one, sum_two, total_one, total_two, out):
    value = squares(held_one, arrived_one, total_one) + squares(held_two, arrived_two, total_two)

    @pl.when(pl.program_id(0) == 0)
    def _():
        out[...] = jnp.broadcast_to(jnp.sum(sum_one[...] + sum_two[...], axis=0, keepdims=True), out.shape)

    out[...] += jnp.broadcast_to(jnp.sum(value, axis=0, keepdims=True), out.shape)


def short_squares(lays, helds, arriveds, sums, devices):
    tile = pl.BlockSpec((8, 128), lambda i: (0, 0))
    one, two = lays
    *totals, sums = call(
        short_body,
        HEAD,
        [one.shard(), one.shard(), two.shard(), two.shard(), tile, tile],
        [one.shard(), two.shard(), pl.BlockSpec((devices, 128), lambda i: (0, 0))],
        [lay.array(HEAD, jnp.float32) for lay in lays] + [jax.ShapeDtypeStruct((devices, 128), jnp.float32)],
        one.bytes(HEAD, 20),
    )(helds[0], arriveds[0], helds[1], arriveds[1], *sums)
    return totals, sums


def clip_of(entries, sums):
    sumsq = jnp.sum(jnp.sum(sums[...], axis=0, keepdims=True), axis=1, keepdims=True)
    return jnp.minimum(1.0, lax.rsqrt(sumsq / entries + 1e-06))


def weight_body(entries, sums, total, kept, pull, spread, out):
    scaled = clip_of(entries, sums) * total[...]
    out[...] = shard_of(kept[...], pull[...], spread[...], scaled).astype(jnp.bfloat16)


def weight_tail(lay, entries, sums, total, terms):
    n = BLOCKS - HEAD
    return call(
        functools.partial(weight_body, entries),
        n,
        [pl.BlockSpec(sums.shape, lambda i: (0, 0)), lay.shard()] + [lay.shard(HEAD)] * 3,
        lay.shard(),
        lay.array(n, jnp.bfloat16),
        lay.bytes(n, 18),
    )(sums, total, *terms)


def weight_whole(lay, entries, sums, short, long, terms):
    return call(
        functools.partial(weight_whole_body, entries),
        BLOCKS,
        [pl.BlockSpec(sums.shape, lambda i: (0, 0)), lay.short(), lay.long()] + [lay.shard()] * 3,
        lay.shard(),
        lay.array(BLOCKS, jnp.bfloat16),
        lay.bytes(BLOCKS, 22),
    )(sums, short, long, *terms)


def weight_whole_body(entries, sums, short, long, kept, pull, spread, out):
    scaled = clip_of(entries, sums) * jnp.where(pl.program_id(0) < HEAD, short[...], long[...])
    out[...] = shard_of(kept[...], pull[...], spread[...], scaled).astype(jnp.bfloat16)


def weight_heads_body(entries, sums, *refs):
    clip = clip_of(entries, sums)
    for (total, kept, pull, spread), out in zip((refs[:4], refs[4:8]), refs[8:]):
        out[...] = shard_of(kept[...], pull[...], spread[...], clip * total[...]).astype(jnp.bfloat16)


def weight_heads(lays, entries, sums, totals, terms):
    one, two = lays
    return call(
        functools.partial(weight_heads_body, entries),
        HEAD,
        [pl.BlockSpec(sums.shape, lambda i: (0, 0))] + [one.shard()] * 4 + [two.shard()] * 4,
        [one.shard(), two.shard()],
        [lay.array(HEAD, jnp.bfloat16) for lay in lays],
        one.bytes(HEAD, 36),
    )(sums, totals[0], *terms[0], totals[1], *terms[1])


def update_body(entries, sums, short, long, master, moment, second, shard_out, first_out, variance_out):
    scaled = clip_of(entries, sums) * jnp.where(pl.program_id(0) < HEAD, short[...], long[...])
    shard_out[...] = shard_of(
        KEEP * master[...], (FIRST * beta_one) * moment[...], (SECOND * beta_two) * second[...], scaled
    )
    first_out[...] = beta_one * moment[...] + (1.0 - beta_one) * scaled
    variance_out[...] = beta_two * second[...] + (1.0 - beta_two) * (scaled * scaled)


def update(lay, entries, sums, short, long, state):
    return call(
        functools.partial(update_body, entries),
        BLOCKS,
        [pl.BlockSpec(sums.shape, lambda i: (0, 0)), lay.short(), lay.long()] + [lay.shard()] * 3,
        [lay.shard()] * 3,
        [lay.array(BLOCKS, jnp.float32)] * 3,
        lay.bytes(BLOCKS, 28),
    )(sums, short, long, *state)


def place_body(_, short, long, out):
    out[...] = jnp.where(pl.program_id(0) < HEAD, short[...], long[...])


def place(lay, whole, short, long, partner):
    return call(
        place_body,
        BLOCKS,
        [pl.BlockSpec(memory_space=pl.ANY), lay.short(), lay.long()],
        lay.piece(partner),
        jax.ShapeDtypeStruct(lay.whole, jnp.bfloat16),
        lay.bytes(BLOCKS, 4),
        aliases={0: 0},
    )(whole, short, long)


def place_whole_body(*refs):
    refs[-1][...] = refs[-2][...]


def place_whole(lay, whole, piece, partner):
    first = whole is None
    return call(
        place_whole_body,
        BLOCKS,
        ([] if first else [pl.BlockSpec(memory_space=pl.ANY)]) + [lay.shard()],
        lay.piece(partner),
        jax.ShapeDtypeStruct(lay.whole, jnp.bfloat16),
        lay.bytes(BLOCKS, 4),
        aliases=None if first else {0: 0},
    )(*([] if first else [whole]), piece)


def place_long_body(_, long, out):
    out[...] = long[...]


def place_long(lay, whole, long, partner):
    return call(
        place_long_body,
        BLOCKS - HEAD,
        [pl.BlockSpec(memory_space=pl.ANY), lay.shard()],
        lay.piece(partner, HEAD),
        jax.ShapeDtypeStruct(lay.whole, jnp.bfloat16),
        lay.bytes(BLOCKS - HEAD, 4),
        aliases={0: 0},
    )(whole, long)


def place_heads_body(lays, partner, _, __, one, two, out_one, out_two, sems):
    owner = lax.axis_index("dp") ^ partner
    copies = []
    for k, (lay, head, out) in enumerate(zip(lays, (one, two), (out_one, out_two))):
        target = lay.quarter(out, owner, 0, HEAD)
        copies.append(pltpu.make_async_copy(head, target, sems.at[k]))
    for copy in copies:
        copy.start()
    for copy in copies:
        copy.wait()


def place_heads(lays, wholes, heads, partner):
    size = sum(lay.bytes(HEAD, 2) for lay in lays)
    return pl.pallas_call(
        functools.partial(place_heads_body, lays, partner),
        in_specs=[pl.BlockSpec(memory_space=pl.ANY)] * 4,
        out_specs=[pl.BlockSpec(memory_space=pl.ANY)] * 2,
        out_shape=[jax.ShapeDtypeStruct(lay.whole, jnp.bfloat16) for lay in lays],
        scratch_shapes=[pltpu.SemaphoreType.DMA((2,))],
        input_output_aliases={0: 0, 1: 1},
        compiler_params=pltpu.CompilerParams(vmem_limit_bytes=CUT_GRANT * 2**20),
        cost_estimate=pl.CostEstimate(flops=size, bytes_accessed=2 * size, transcendentals=0),
        name="place_heads",
    )(*wholes, *heads)


def exchange(value, partner, parts):
    return lax.ppermute(value, "dp", [(i, i ^ partner) for i in range(parts)])


def on_square(parts, devices, entries, *args):
    grads = [a.reshape(a.shape[-2:]) for a in args[:2]]
    accums = [a.reshape(a.shape[-2:]) for a in args[2:4]]
    states = [[a.reshape(a.shape[-2:]) for a in args[4 + k :: 2]] for k in range(2)]
    lays = [Layout(*accums[k].shape, k, parts) for k in range(2)]
    near, far = (1, 2), (2, 1)
    both = range(2)

    def step(function, *lists):
        return [function(lays[k], *(x[k] for x in lists)) for k in both]

    def move(values, partners):
        return [exchange(values[k], partners[k], parts) for k in both]

    relay_head = move(cut(lays, grads, (3, 3), 0, HEAD), near)
    relay_tail = move(cut(lays, grads, (3, 3), HEAD, BLOCKS - HEAD), near)
    direct = move(cut(lays, grads, near), near)
    sent = step(add_forward, grads, relay_head, relay_tail, far)
    tail = move([x[1] for x in sent], far)
    head = move([x[0] for x in sent], far)
    held = step(partial_sum, grads, direct, accums)
    terms = step(ready, states)
    tail_totals, sums = zip(*step(long_squares, held, tail))
    head_totals, sums = short_squares(lays, held, head, sums, devices)
    sums = lax.all_to_all(sums, ("dp", "mp"), 0, 0, tiled=True)

    own_head = weight_heads(lays, entries, sums, head_totals, terms)
    own_tail = step(lambda lay, *x: weight_tail(lay, entries, sums, *x), tail_totals, terms)
    near_head, near_tail = move(own_head, near), move(own_tail, near)
    own = step(lambda lay, *x: weight_whole(lay, entries, sums, *x), head_totals, tail_totals, terms)
    opposite = move(own, far)
    last_tail, last_head = move(near_tail, far), move(near_head, far)

    updated = step(lambda lay, *x: update(lay, entries, sums, *x), head_totals, tail_totals, states)
    wholes = step(place_whole, (None, None), own, (0, 0))
    wholes = step(place, wholes, near_head, near_tail, near)
    wholes = step(place_whole, wholes, opposite, far)
    wholes = step(place_long, wholes, last_tail, (3, 3))
    wholes = place_heads(lays, wholes, last_head, 3)
    return tuple(w[None] for w in wholes) + tuple(updated[k][j][None] for j in range(3) for k in both)


def on_any(entries, *args):
    grads, accums = args[:2], args[2:4]
    states = [args[4 + k :: 2] for k in range(2)]
    axes = (1, 2)
    totals = [
        accums[k]
        + lax.psum_scatter(grads[k][0], "dp", scatter_dimension=axes[k], tiled=True).astype(jnp.float32)
        for k in range(2)
    ]
    sumsq = lax.psum(sum(jnp.sum(t * t) for t in totals), ("dp", "mp"))
    clip = jnp.minimum(1.0, lax.rsqrt(sumsq / entries + 1e-06))
    updated = [adamw(totals[k], clip, *states[k]) for k in range(2)]
    weights = tuple(
        lax.all_gather(updated[k][0].astype(jnp.bfloat16), "dp", axis=axes[k], tiled=True) for k in range(2)
    )
    return weights + tuple(updated[k][j] for j in range(3) for k in range(2))


def solution(mesh):
    parts = mesh.shape["dp"]
    devices = mesh.size

    def on_device(*args):
        entries = float(devices * sum(a.size for a in args[2:4]))
        tiled = all(a.shape[-2] % (16 * BLOCKS) == 0 and a.shape[-1] % 128 == 0 for a in args[2:4])
        if parts == 4 and tiled:
            return on_square(parts, devices, entries, *args)
        return on_any(entries, *args)

    rows, cols = P(None, "dp", "mp"), P(None, "mp", "dp")
    return jax.shard_map(
        on_device,
        mesh=mesh,
        in_specs=(P("dp", None, None, "mp"), P("dp", None, "mp", None)) + (rows, cols) * 4,
        out_specs=(P(None, None, "mp"), P(None, "mp", None)) + (rows, cols) * 3,
        check_vma=False,
    )
```

```python
import functools

import jax
import jax.numpy as jnp
from jax import lax
from jax.experimental import pallas as pl
from jax.experimental.pallas import tpu as pltpu
from jax.sharding import PartitionSpec as P


STEP = 10

beta_one = 0.9
beta_two = 0.95
learn_rate = 0.002
weight_decay = 0.1
adam_eps = 1e-08

BLOCKS = 4
HEAD = 1

CUT_GRANT = 8


def adamw(total, clip, master, moment, second):
    scaled = clip * total
    first = beta_one * moment + (1.0 - beta_one) * scaled
    variance = beta_two * second + (1.0 - beta_two) * scaled * scaled
    corr_one = 1.0 - beta_one**STEP
    corr_two = 1.0 - beta_two**STEP
    update = first * (1.0 / corr_one) / (jnp.sqrt(variance * (1.0 / corr_two)) + adam_eps)
    return (master - learn_rate * (update + weight_decay * master), first, variance)


KEEP = 1.0 - learn_rate * weight_decay
ROOT = ((1.0 - beta_two) / (1.0 - beta_two**STEP)) ** 0.5
PULL = learn_rate / (1.0 - beta_one**STEP) * beta_one / ROOT
PUSH = learn_rate / (1.0 - beta_one**STEP) * (1.0 - beta_one) / ROOT
SPREAD = beta_two / (1.0 - beta_two)
EDGE = adam_eps / ROOT


def shard_of(kept, pull, spread, scaled):
    square = spread + scaled * scaled
    return kept - (pull + PUSH * scaled) / (square * lax.rsqrt(square) + EDGE)


class Layout:
    def __init__(self, rows, cols, axis, parts):
        self.rows, self.cols, self.axis, self.parts = rows, cols, axis, parts
        self.step = rows // BLOCKS
        self.block = (self.step, cols)
        self.whole = (rows * parts, cols) if axis == 0 else (rows, cols * parts)

    def piece(self, partner, start=0):
        def index(i):
            owner = lax.axis_index("dp") ^ partner
            return (owner * BLOCKS + start + i, 0) if self.axis == 0 else (start + i, owner)

        return pl.BlockSpec(self.block, index)

    def quarter(self, ref, owner, start=0, blocks=BLOCKS):
        first, size = start * self.step, blocks * self.step
        if self.axis == 0:
            return ref.at[pl.ds(pl.multiple_of(owner * self.rows + first, self.step), size), :]
        return ref.at[pl.ds(first, size), pl.ds(pl.multiple_of(owner * self.cols, self.cols), self.cols)]

    def shard(self, start=0):
        return pl.BlockSpec(self.block, lambda i: (start + i, 0))

    def short(self):
        return pl.BlockSpec(self.block, lambda i: (jnp.minimum(i, HEAD - 1), 0))

    def long(self):
        return pl.BlockSpec(self.block, lambda i: (jnp.maximum(i - HEAD, 0), 0))

    def array(self, blocks, dtype):
        return jax.ShapeDtypeStruct((blocks * self.step, self.cols), dtype)

    def bytes(self, blocks, width):
        return blocks * self.step * self.cols * width


def call(body, grid, in_specs, out_specs, out_shape, cost, aliases=None, grant=24):
    return pl.pallas_call(
        body,
        grid=(grid,),
        in_specs=in_specs,
        out_specs=out_specs,
        out_shape=out_shape,
        input_output_aliases=aliases or {},
        compiler_params=pltpu.CompilerParams(
            dimension_semantics=("arbitrary",), vmem_limit_bytes=grant * 2**20
        ),
        cost_estimate=pl.CostEstimate(flops=cost * 2, bytes_accessed=cost, transcendentals=0),
    )


def cut_body(lays, partners, start, blocks, grads_one, grads_two, out_one, out_two, sems):
    me = lax.axis_index("dp")
    copies = [
        pltpu.make_async_copy(lay.quarter(grads, me ^ partner, start, blocks), out, sems.at[k])
        for k, (lay, partner, grads, out) in enumerate(
            zip(lays, partners, (grads_one, grads_two), (out_one, out_two))
        )
    ]
    for copy in copies:
        copy.start()
    for copy in copies:
        copy.wait()


def cut(lays, grads, partners, start=0, blocks=BLOCKS):
    size = sum(lay.bytes(blocks, 2) for lay in lays)
    return pl.pallas_call(
        functools.partial(cut_body, lays, partners, start, blocks),
        in_specs=[pl.BlockSpec(memory_space=pltpu.HBM)] * 2,
        out_specs=[pl.BlockSpec(memory_space=pl.ANY)] * 2,
        out_shape=[pltpu.VMEM((blocks * lay.step, lay.cols), jnp.bfloat16) for lay in lays],
        scratch_shapes=[pltpu.SemaphoreType.DMA((2,))],
        compiler_params=pltpu.CompilerParams(vmem_limit_bytes=CUT_GRANT * 2**20),
        cost_estimate=pl.CostEstimate(flops=size, bytes_accessed=2 * size, transcendentals=0),
        name="cut",
    )(*(pltpu.with_memory_space_constraint(g, pltpu.HBM) for g in grads))


def add_body(grads, arrived_short, arrived_long, short, long):
    i = pl.program_id(0)
    arrived = jnp.where(i < HEAD, arrived_short[...].astype(jnp.float32), arrived_long[...].astype(jnp.float32))
    value = (grads[...].astype(jnp.float32) + arrived).astype(jnp.bfloat16)

    @pl.when(i < HEAD)
    def _():
        short[...] = value

    @pl.when(i >= HEAD)
    def _():
        long[...] = value


def add_forward(lay, grads, short, long, partner):
    return call(
        add_body,
        BLOCKS,
        [lay.piece(partner), lay.short(), lay.long()],
        [lay.short(), lay.long()],
        [lay.array(HEAD, jnp.bfloat16), lay.array(BLOCKS - HEAD, jnp.bfloat16)],
        lay.bytes(BLOCKS, 6),
    )(grads, short, long)


def partial_body(grads, arrived, accum, out):
    out[...] = accum[...] + (grads[...].astype(jnp.float32) + arrived[...].astype(jnp.float32))


def partial_sum(lay, grads, arrived, accum):
    return call(
        partial_body,
        BLOCKS,
        [lay.piece(0), lay.shard(), lay.shard()],
        lay.shard(),
        lay.array(BLOCKS, jnp.float32),
        lay.bytes(BLOCKS, 12),
    )(grads, arrived, accum)


def ready_body(master, moment, second, kept, pull, spread):
    kept[...] = KEEP * master[...]
    pull[...] = PULL * moment[...]
    spread[...] = SPREAD * second[...]


def ready(lay, state):
    return call(
        ready_body,
        BLOCKS,
        [lay.shard()] * 3,
        [lay.shard()] * 3,
        [lay.array(BLOCKS, jnp.float32)] * 3,
        lay.bytes(BLOCKS, 24),
    )(*state)


def squares(held, arrived, out):
    total = held[...] + arrived[...].astype(jnp.float32)
    out[...] = total
    rows, cols = total.shape
    tile = jnp.sum((total * total).reshape(rows // 8, 8, cols), axis=0)
    return sum(tile[:, k : k + 128] for k in range(0, cols, 128))


def long_body(held, arrived, total, out):
    @pl.when(pl.program_id(0) == 0)
    def _():
        out[...] = jnp.zeros_like(out)

    out[...] += squares(held, arrived, total)


def long_squares(lay, held, arrived):
    n = BLOCKS - HEAD
    return call(
        long_body,
        n,
        [lay.shard(HEAD), lay.shard()],
        [lay.shard(), pl.BlockSpec((8, 128), lambda i: (0, 0))],
        [lay.array(n, jnp.float32), jax.ShapeDtypeStruct((8, 128), jnp.float32)],
        lay.bytes(n, 10),
    )(held, arrived)


def short_body(held_one, arrived_one, held_two, arrived_two, sum_one, sum_two, total_one, total_two, out):
    value = squares(held_one, arrived_one, total_one) + squares(held_two, arrived_two, total_two)

    @pl.when(pl.program_id(0) == 0)
    def _():
        out[...] = jnp.broadcast_to(jnp.sum(sum_one[...] + sum_two[...], axis=0, keepdims=True), out.shape)

    out[...] += jnp.broadcast_to(jnp.sum(value, axis=0, keepdims=True), out.shape)


def short_squares(lays, helds, arriveds, sums, devices):
    tile = pl.BlockSpec((8, 128), lambda i: (0, 0))
    one, two = lays
    *totals, sums = call(
        short_body,
        HEAD,
        [one.shard(), one.shard(), two.shard(), two.shard(), tile, tile],
        [one.shard(), two.shard(), pl.BlockSpec((devices, 128), lambda i: (0, 0))],
        [lay.array(HEAD, jnp.float32) for lay in lays] + [jax.ShapeDtypeStruct((devices, 128), jnp.float32)],
        one.bytes(HEAD, 20),
    )(helds[0], arriveds[0], helds[1], arriveds[1], *sums)
    return totals, sums


def clip_of(entries, sums):
    sumsq = jnp.sum(jnp.sum(sums[...], axis=0, keepdims=True), axis=1, keepdims=True)
    return jnp.minimum(1.0, lax.rsqrt(sumsq / entries + 1e-06))


def weight_body(entries, sums, total, kept, pull, spread, out):
    scaled = clip_of(entries, sums) * total[...]
    out[...] = shard_of(kept[...], pull[...], spread[...], scaled).astype(jnp.bfloat16)


def weight_tail(lay, entries, sums, total, terms):
    n = BLOCKS - HEAD
    return call(
        functools.partial(weight_body, entries),
        n,
        [pl.BlockSpec(sums.shape, lambda i: (0, 0)), lay.shard()] + [lay.shard(HEAD)] * 3,
        lay.shard(),
        lay.array(n, jnp.bfloat16),
        lay.bytes(n, 18),
    )(sums, total, *terms)


def weight_whole(lay, entries, sums, short, long, terms):
    return call(
        functools.partial(weight_whole_body, entries),
        BLOCKS,
        [pl.BlockSpec(sums.shape, lambda i: (0, 0)), lay.short(), lay.long()] + [lay.shard()] * 3,
        lay.shard(),
        lay.array(BLOCKS, jnp.bfloat16),
        lay.bytes(BLOCKS, 22),
    )(sums, short, long, *terms)


def weight_whole_body(entries, sums, short, long, kept, pull, spread, out):
    scaled = clip_of(entries, sums) * jnp.where(pl.program_id(0) < HEAD, short[...], long[...])
    out[...] = shard_of(kept[...], pull[...], spread[...], scaled).astype(jnp.bfloat16)


def weight_heads_body(entries, sums, *refs):
    clip = clip_of(entries, sums)
    for (total, kept, pull, spread), out in zip((refs[:4], refs[4:8]), refs[8:]):
        out[...] = shard_of(kept[...], pull[...], spread[...], clip * total[...]).astype(jnp.bfloat16)


def weight_heads(lays, entries, sums, totals, terms):
    one, two = lays
    return call(
        functools.partial(weight_heads_body, entries),
        HEAD,
        [pl.BlockSpec(sums.shape, lambda i: (0, 0))] + [one.shard()] * 4 + [two.shard()] * 4,
        [one.shard(), two.shard()],
        [lay.array(HEAD, jnp.bfloat16) for lay in lays],
        one.bytes(HEAD, 36),
    )(sums, totals[0], *terms[0], totals[1], *terms[1])


def update_body(entries, sums, short, long, master, moment, second, shard_out, first_out, variance_out):
    scaled = clip_of(entries, sums) * jnp.where(pl.program_id(0) < HEAD, short[...], long[...])
    shard_out[...] = shard_of(
        KEEP * master[...], PULL * moment[...], SPREAD * second[...], scaled
    )
    first_out[...] = beta_one * moment[...] + (1.0 - beta_one) * scaled
    variance_out[...] = beta_two * second[...] + (1.0 - beta_two) * (scaled * scaled)


def update(lay, entries, sums, short, long, state):
    return call(
        functools.partial(update_body, entries),
        BLOCKS,
        [pl.BlockSpec(sums.shape, lambda i: (0, 0)), lay.short(), lay.long()] + [lay.shard()] * 3,
        [lay.shard()] * 3,
        [lay.array(BLOCKS, jnp.float32)] * 3,
        lay.bytes(BLOCKS, 28),
    )(sums, short, long, *state)


def place_body(_, short, long, out):
    out[...] = jnp.where(pl.program_id(0) < HEAD, short[...], long[...])


def place(lay, whole, short, long, partner):
    return call(
        place_body,
        BLOCKS,
        [pl.BlockSpec(memory_space=pl.ANY), lay.short(), lay.long()],
        lay.piece(partner),
        jax.ShapeDtypeStruct(lay.whole, jnp.bfloat16),
        lay.bytes(BLOCKS, 4),
        aliases={0: 0},
    )(whole, short, long)


def place_whole_body(*refs):
    refs[-1][...] = refs[-2][...]


def place_whole(lay, whole, piece, partner):
    first = whole is None
    return call(
        place_whole_body,
        BLOCKS,
        ([] if first else [pl.BlockSpec(memory_space=pl.ANY)]) + [lay.shard()],
        lay.piece(partner),
        jax.ShapeDtypeStruct(lay.whole, jnp.bfloat16),
        lay.bytes(BLOCKS, 4),
        aliases=None if first else {0: 0},
    )(*([] if first else [whole]), piece)


def place_long_body(_, long, out):
    out[...] = long[...]


def place_long(lay, whole, long, partner):
    return call(
        place_long_body,
        BLOCKS - HEAD,
        [pl.BlockSpec(memory_space=pl.ANY), lay.shard()],
        lay.piece(partner, HEAD),
        jax.ShapeDtypeStruct(lay.whole, jnp.bfloat16),
        lay.bytes(BLOCKS - HEAD, 4),
        aliases={0: 0},
    )(whole, long)


def place_heads_body(lays, partner, _, __, one, two, out_one, out_two, sems):
    owner = lax.axis_index("dp") ^ partner
    copies = []
    for k, (lay, head, out) in enumerate(zip(lays, (one, two), (out_one, out_two))):
        target = lay.quarter(out, owner, 0, HEAD)
        copies.append(pltpu.make_async_copy(head, target, sems.at[k]))
    for copy in copies:
        copy.start()
    for copy in copies:
        copy.wait()


def place_heads(lays, wholes, heads, partner):
    size = sum(lay.bytes(HEAD, 2) for lay in lays)
    return pl.pallas_call(
        functools.partial(place_heads_body, lays, partner),
        in_specs=[pl.BlockSpec(memory_space=pl.ANY)] * 4,
        out_specs=[pl.BlockSpec(memory_space=pl.ANY)] * 2,
        out_shape=[jax.ShapeDtypeStruct(lay.whole, jnp.bfloat16) for lay in lays],
        scratch_shapes=[pltpu.SemaphoreType.DMA((2,))],
        input_output_aliases={0: 0, 1: 1},
        compiler_params=pltpu.CompilerParams(vmem_limit_bytes=CUT_GRANT * 2**20),
        cost_estimate=pl.CostEstimate(flops=size, bytes_accessed=2 * size, transcendentals=0),
        name="place_heads",
    )(*wholes, *heads)


def exchange(value, partner, parts):
    return lax.ppermute(value, "dp", [(i, i ^ partner) for i in range(parts)])


def on_square(parts, devices, entries, *args):
    grads = [a.reshape(a.shape[-2:]) for a in args[:2]]
    accums = [a.reshape(a.shape[-2:]) for a in args[2:4]]
    states = [[a.reshape(a.shape[-2:]) for a in args[4 + k :: 2]] for k in range(2)]
    lays = [Layout(*accums[k].shape, k, parts) for k in range(2)]
    near, far = (1, 2), (2, 1)
    both = range(2)

    def step(function, *lists):
        return [function(lays[k], *(x[k] for x in lists)) for k in both]

    def move(values, partners):
        return [exchange(values[k], partners[k], parts) for k in both]

    relay_head = move(cut(lays, grads, (3, 3), 0, HEAD), near)
    relay_tail = move(cut(lays, grads, (3, 3), HEAD, BLOCKS - HEAD), near)
    direct = move(cut(lays, grads, near), near)
    sent = step(add_forward, grads, relay_head, relay_tail, far)
    tail = move([x[1] for x in sent], far)
    head = move([x[0] for x in sent], far)
    held = step(partial_sum, grads, direct, accums)
    terms = step(ready, states)
    tail_totals, sums = zip(*step(long_squares, held, tail))
    head_totals, sums = short_squares(lays, held, head, sums, devices)
    sums = lax.all_to_all(sums, ("dp", "mp"), 0, 0, tiled=True)

    own_head = weight_heads(lays, entries, sums, head_totals, terms)
    own_tail = step(lambda lay, *x: weight_tail(lay, entries, sums, *x), tail_totals, terms)
    near_head, near_tail = move(own_head, near), move(own_tail, near)
    own = step(lambda lay, *x: weight_whole(lay, entries, sums, *x), head_totals, tail_totals, terms)
    opposite = move(own, far)
    last_tail, last_head = move(near_tail, far), move(near_head, far)

    updated = step(lambda lay, *x: update(lay, entries, sums, *x), head_totals, tail_totals, states)
    wholes = step(place_whole, (None, None), own, (0, 0))
    wholes = step(place, wholes, near_head, near_tail, near)
    wholes = step(place_whole, wholes, opposite, far)
    wholes = step(place_long, wholes, last_tail, (3, 3))
    wholes = place_heads(lays, wholes, last_head, 3)
    return tuple(w[None] for w in wholes) + tuple(updated[k][j][None] for j in range(3) for k in both)


def on_any(entries, *args):
    grads, accums = args[:2], args[2:4]
    states = [args[4 + k :: 2] for k in range(2)]
    axes = (1, 2)
    totals = [
        accums[k]
        + lax.psum_scatter(grads[k][0], "dp", scatter_dimension=axes[k], tiled=True).astype(jnp.float32)
        for k in range(2)
    ]
    sumsq = lax.psum(sum(jnp.sum(t * t) for t in totals), ("dp", "mp"))
    clip = jnp.minimum(1.0, lax.rsqrt(sumsq / entries + 1e-06))
    updated = [adamw(totals[k], clip, *states[k]) for k in range(2)]
    weights = tuple(
        lax.all_gather(updated[k][0].astype(jnp.bfloat16), "dp", axis=axes[k], tiled=True) for k in range(2)
    )
    return weights + tuple(updated[k][j] for j in range(3) for k in range(2))


def solution(mesh):
    parts = mesh.shape["dp"]
    devices = mesh.size

    def on_device(*args):
        entries = float(devices * sum(a.size for a in args[2:4]))
        tiled = all(a.shape[-2] % (16 * BLOCKS) == 0 and a.shape[-1] % 128 == 0 for a in args[2:4])
        if parts == 4 and tiled:
            return on_square(parts, devices, entries, *args)
        return on_any(entries, *args)

    rows, cols = P(None, "dp", "mp"), P(None, "mp", "dp")
    return jax.shard_map(
        on_device,
        mesh=mesh,
        in_specs=(P("dp", None, None, "mp"), P("dp", None, "mp", None)) + (rows, cols) * 4,
        out_specs=(P(None, None, "mp"), P(None, "mp", None)) + (rows, cols) * 3,
        check_vma=False,
    )
```
